256 devices in a mesh: row: 16 (over x_hi, y, core), col: 16 (over x_lo, z).
Axes of the slice: x: 4 (x_hi: 2, x_lo: 2; x = x_hi * 2 + x_lo), y: 4, z: 8, core: 2. Of those that a mesh axis runs over, the one named last changes fastest.
Arguments:
- gradient: float32 [4096, 4608], P('row', 'col'), may hold values from -12 to 12
- first_moment: float32 [4096, 4608], P('row', 'col'), may hold values from -12 to 12, as said below
- second_moment: float32 [4096, 4608], P('row', 'col'), may hold values from 0.01 to 1
- weights: float32 [4096, 4608], P('row', 'col'), may hold values from -6 to 6
- eigenbasis: float32 [4608, 4608], P('row', 'col'), may hold values from -1 to 1, as said below
Outputs:
- new_weights: float32 [4096, 4608], P('row', 'col')
- new_first: float32 [4096, 4608], P('row', 'col')
- new_second: float32 [4096, 4608], P('row', 'col')
The draws below stay inside these ranges and needn't reach their ends.
Inputs may be any that keep to these rules, and one draw needn't show every extreme that they name: `first_moment`: every entry's magnitude is at most 12. eigenbasis is orthogonal: its columns are orthonormal.
All inputs are finite; a program needn't handle non-finite values.
Results may differ from the reference program's by a relative error of at most 0.000059.
Values sent between devices are 32-bit elements; how exact they have to be, the bound alone decides.
A program may use at most 64 MiB of HBM per device.

```python
import math
import jax
import jax.numpy as jnp
from jax import lax

D = 4608
VOCAB = 4096


def draw_first_moment(key, part):
    key_rows = jax.random.fold_in(key, 11)
    key_cells = jax.random.fold_in(key, 12)
    row_factor = jnp.exp(jax.random.uniform(key_rows, (VOCAB, 1), jnp.float32, jnp.log(0.3), jnp.log(3.0)))
    cells = jax.random.truncated_normal(key_cells, -4.0, 4.0, (VOCAB, D), jnp.float32)
    return (cells * row_factor).astype(jnp.float32)


def draw_eigenbasis(key, part):
    key_basis = jax.random.fold_in(key, 21)
    source = jax.random.normal(key_basis, (D, D), jnp.float32)
    orthogonal, upper = jnp.linalg.qr(source)
    return orthogonal.astype(jnp.float32)


def steps_of(own_key, dims, cuts, least, largest):
    level = 1.0
    for position, shards_of in cuts:
        heights = jax.random.uniform(jax.random.fold_in(jax.random.fold_in(own_key, 6), position), (shards_of,), jnp.float32, least / len(cuts), largest / len(cuts))
        level = level * jnp.repeat(jnp.exp(heights), dims[position] // shards_of).reshape((-1,) + (1,) * (len(dims) - 1 - position))
    return level


def gaussian(stream_key, shape, spread, bound, split=(), dtype=jnp.bfloat16):
    drawn = spread * jax.random.normal(stream_key, shape, jnp.float32)
    if split:
        drawn = drawn * steps_of(stream_key, shape, split, -0.22, 0.18)
    return jnp.clip(drawn, -bound, bound).astype(dtype)


def setup_inputs(seed: int = 0) -> dict:
    keys = jax.random.split(jax.random.key(seed), 6)
    gradient = gaussian(keys[0], (VOCAB, D), 2.0, 12.0, ((0, 16), (1, 16)), jnp.float32)
    first_moment = draw_first_moment(jax.random.fold_in(keys[5], 71), 0)
    second_moment = jnp.clip(jnp.exp(math.log(1.0) - 4.6051702 * jax.random.uniform(keys[2], (VOCAB, D), jnp.float32) ** steps_of(keys[2], (VOCAB, D), ((0, 16), (1, 16)), -0.2, 0.2)), 0.01, 1.0)
    weights = gaussian(keys[3], (VOCAB, D), 1.0, 6.0, ((0, 16), (1, 16)), jnp.float32)
    eigenbasis = draw_eigenbasis(jax.random.fold_in(keys[5], 71), 0)
    return dict(gradient=gradient, first_moment=first_moment, second_moment=second_moment, weights=weights, eigenbasis=eigenbasis)


bias_first = 1.0 - 0.9 ** 10
bias_second = 1.0 - 0.999 ** 10
epsilon = 1e-08
step_rate = 0.25

def reference(gradient, first_moment, second_moment, weights, eigenbasis):
    highest = lax.Precision.HIGHEST
    rotated = jnp.dot(gradient.astype(jnp.float32), eigenbasis.astype(jnp.float32), precision=highest, preferred_element_type=jnp.float32)
    new_first = 0.9 * first_moment + 0.1 * rotated
    new_second = 0.999 * second_moment + 0.001 * rotated * rotated
    direction = new_first / bias_first / (jnp.sqrt(new_second / bias_second) + epsilon)
    row_rms = jnp.sqrt(lax.optimization_barrier(jnp.sum(direction * direction, axis=1, keepdims=True)) / D)
    update = jnp.dot(direction.astype(jnp.float32), eigenbasis.T.astype(jnp.float32), precision=highest, preferred_element_type=jnp.float32)
    new_weights = weights - step_rate * update / jnp.maximum(1.0, row_rms)
    return (new_weights, new_first, new_second)
```

```python
import jax
import jax.numpy as jnp
from jax import lax
from jax.experimental import pallas as pl
from jax.experimental.pallas import tpu as pltpu
from jax.sharding import PartitionSpec as P

MESH = pl.DeviceIdType.MESH
D = 4608
bias_first = 1.0 - 0.9**10
bias_second = 1.0 - 0.999**10
epsilon = 1e-08
step_rate = 0.25

B = 288
M = 256
NB = 16
Q_HALF = ((0, 328), (328, 320))
G_HALF = ((0, 144), (144, 144))
U_HALF = ((0, 152), (152, 144))
NSEND = 128


def split(v):
    hi = v.astype(jnp.bfloat16)
    return hi, (v - hi.astype(jnp.float32)).astype(jnp.bfloat16)


def dot3(ah, al, bh, bl, dims):
    def one(p, q):
        return lax.dot_general(p, q, (dims, ((), ())), preferred_element_type=jnp.float32)

    return one(ah, bh) + (one(ah, bl) + one(al, bh))


def kernel(g, q, m1, m2, rot_o, upd_o, gbuf, qbuf, qstage, qh, ql, mbuf, acc, ustage, dh, dl, osend, ubuf, dbuf, rbuf, ss, qs, gs, ms, ds, rs, us):
    row, col = lax.axis_index("row"), lax.axis_index("col")
    xh, y, b = row // 8, lax.rem(row // 2, 4), lax.rem(row, 2)
    a, z = col // 8, lax.rem(col, 8)
    x = 2 * xh + a
    o = 1 - b
    cond = {"S": a == b, "N": a != b}
    xp, xm = lax.rem(x + 1, 4), lax.rem(x + 3, 4)
    yy = {d: lax.rem(y + d + 4, 4) for d in (0, 1, -1, 2)}
    zz = {d: lax.rem(z + d + 8, 8) for d in range(-4, 5)}

    def dev(x_, y_, z_, c_):
        return ((x_ // 2) * 8 + y_ * 2 + c_, lax.rem(x_, 2) * 8 + z_)

    to = {
        "x+": dev(xp, y, z, b),
        "x-": dev(xm, y, z, b),
        "y+": dev(x, yy[1], z, b),
        "y-": dev(x, yy[-1], z, b),
        "z+": dev(x, y, zz[1], b),
        "z-": dev(x, y, zz[-1], b),
        "core": dev(x, y, z, o),
        "swap": dev(2 * xh + b, y, z, o),
    }

    def on(tag, f):
        if tag is None:
            f()
        else:
            pl.when(cond[tag])(f)

    sends = []

    def send(tag, src, dst, rsem, where):
        k = len(sends)

        def make():
            return pltpu.make_async_remote_copy(
                src_ref=src(), dst_ref=dst(), send_sem=ss.at[k], recv_sem=rsem(), device_id=to[where], device_id_type=MESH
            )

        make().start()
        sends.append((tag, make))

    def arrived(ref, sem):
        pltpu.make_async_copy(ref, ref, sem).wait()

    def blk(h, d, c):
        return h * 8 + yy[d] * 2 + c

    def q_part(i, half):
        return qbuf.at[i, pl.ds(*Q_HALF[half]), :]

    def q_send(tag, i, half, *wheres):
        for w in wheres:
            send(tag, lambda: q_part(i(), half), lambda: q_part(i(), half), lambda: qs.at[i(), half], w)

    def q_wait(i, half):
        arrived(q_part(i(), half), qs.at[i(), half])

    def g_part(c, d, half):
        return gbuf.at[c * 8 + zz[d], pl.ds(*G_HALF[half]), :]

    def g_send(tag, d, half, *wheres, src=None):
        for w in wheres:
            s = (lambda: g.at[pl.ds(*G_HALF[half]), :]) if src else (lambda: g_part(b, d, half))
            send(tag, s, lambda: g_part(b, d, half), lambda: gs.at[b * 8 + zz[d], half], w)

    def g_wait(c, d, half):
        arrived(g_part(c, d, half), gs.at[c * 8 + zz[d], half])

    def pack(put):
        put(0, B, q[:, 0:128])
        put(B, B, q[:, 128:256])
        put(2 * B, 72, jnp.concatenate([q[72 * i : 72 * i + 72, 256:288] for i in range(4)], axis=1))

    def pack_own():
        def put(at, n, v):
            qbuf[row, at : at + n, :] = v

        pack(put)

    def pack_stage():
        def put(at, n, v):
            qstage[at : at + n, :] = v

        pack(put)

    barrier = pltpu.get_barrier_semaphore()
    for w in ("x+", "x-", "y+", "y-", "z+", "z-", "core"):
        pl.semaphore_signal(barrier, inc=1, device_id=to[w], device_id_type=MESH)

    @pl.when(cond["N"])
    def _():
        pl.semaphore_signal(barrier, inc=1, device_id=to["swap"], device_id_type=MESH)

    on("S", pack_own)
    on("N", pack_stage)
    on("S", lambda: pl.semaphore_wait(barrier, 7))
    on("N", lambda: pl.semaphore_wait(barrier, 8))

    own = lambda: row
    mate = lambda: blk(xh, 0, o)
    far = lambda d, c: (lambda: blk(1 - xh, d, c))
    left = lambda d, c: (lambda: blk(xm // 2, d, c))
    right = lambda d, c: (lambda: blk(xp // 2, d, c))
    mine = lambda d, c: (lambda: blk(xh, d, c))

    def local(k, half):
        return pltpu.make_async_copy(g.at[pl.ds(*G_HALF[half]), :], g_part(b, 0, half), gs.at[b * 8 + z, half])

    def e0_s():
        for half in (0, 1):
            local(0, half).start()
        q_send("S", own, 0, "x+", "x-")
        q_send("S", own, 1, "y+", "y-")
        for half in (0, 1):
            g_send("S", 0, half, "z+", "z-", "core", src=True)
        pltpu.make_async_copy(m1, mbuf.at[0], ms.at[0]).start()
        pltpu.make_async_copy(m2, mbuf.at[1], ms.at[1]).start()

    def e0_n():
        def hand_q(half):
            send("N", lambda: qstage.at[pl.ds(*Q_HALF[half]), :], lambda: q_part(row, half), lambda: qs.at[row, half], "core")

        def hand_g(half):
            send("N", lambda: g.at[pl.ds(*G_HALF[half]), :], lambda: g_part(o, 0, half), lambda: gs.at[o * 8 + z, half], "swap")

        hand_q(0)
        hand_q(1)
        hand_g(0)
        hand_g(1)

    on("S", e0_s)
    on("N", e0_n)

    def e1_s():
        q_wait(mate, 0)
        q_send("S", mate, 0, "x+", "x-")
        q_wait(mate, 1)
        q_send("S", mate, 1, "y+", "y-")
        for i in (own, mate):
            q_send("S", i, 1, "x+", "x-")
            q_send("S", i, 0, "y+", "y-")

    def z0_n():
        for half in (0, 1):
            g_wait(b, 0, half)
            g_send("N", 0, half, "z+", "z-", "core")

    def e2_n():
        q_wait(left(0, 0), 0)
        q_send("N", left(0, 0), 0, "x+", "y+", "y-")
        q_wait(right(0, 1), 0)
        q_send("N", right(0, 1), 0, "x-", "y+", "y-")
        q_wait(left(0, 1), 0)
        q_send("N", left(0, 1), 0, "y+", "y-")
        q_wait(right(0, 0), 0)
        q_send("N", right(0, 0), 0, "y+", "y-")
        send("N", lambda: m1, lambda: mbuf.at[0], lambda: ms.at[0], "swap")
        send("N", lambda: m2, lambda: mbuf.at[1], lambda: ms.at[1], "swap")

    def e3_s():
        q_wait(mine(-1, 0), 1)
        q_send("S", mine(-1, 0), 1, "y+", "x+", "x-")
        q_wait(mine(1, 1), 1)
        q_send("S", mine(1, 1), 1, "y-", "x+", "x-")
        q_wait(mine(-1, 1), 1)
        q_send("S", mine(-1, 1), 1, "x+", "x-")
        q_wait(mine(1, 0), 1)
        q_send("S", mine(1, 0), 1, "x+", "x-")

    def z_event(d):
        for way, back, first in (("+", -d, 0), ("-", d, 1)):
            for half in (first, 1 - first):
                hops = 4 if half == first else 3
                if d > hops:
                    continue
                g_wait(b, back, half)
                g_send(None, back, half, *((["z" + way] if d < hops else []) + ["core"]))

    def e4_s():
        for c in (0, 1):
            q_wait(far(0, c), 0)
            q_send("S", far(0, c), 0, "y+", "y-")

    def n_b(d, side=None):
        for i, way, c in ((left, "x+", 0), (right, "x-", 1), (left, None, 1), (right, None, 0)):
            q_wait(i(d, c), 1)
            if way:
                q_send("N", i(d, c), 1, way)

    def a_ring():
        for h in (lambda: xh, lambda: 1 - xh):
            for d, way, c in ((-1, "y+", 0), (1, "y-", 1), (-1, None, 1), (1, None, 0)):
                i = lambda h=h, d=d, c=c: blk(h(), d, c)
                q_wait(i, 0)
                if way:
                    q_send(None, i, 0, way)

    def e6_s():
        for c in (0, 1):
            q_wait(mine(2, c), 1)
            q_send("S", mine(2, c), 1, "x+", "x-")

    def s_far(d):
        for c in (0, 1):
            q_wait(far(d, c), 1)

    on("S", e1_s)
    on("N", z0_n)
    on("N", e2_n)
    on("S", e3_s)
    z_event(1)
    on("S", e4_s)
    on("N", lambda: n_b(0))
    z_event(2)
    a_ring()
    on("S", e6_s)
    on("S", lambda: s_far(0))
    z_event(3)

    def n_b1():
        n_b(-1)
        n_b(1)

    on("N", n_b1)
    z_event(4)

    @pl.when(cond["S"])
    def _():
        for half in (0, 1):
            g_wait(b, 0, half)
        s_far(1)
        s_far(-1)

    for d in (0, 1, -1, 2, -2, 3, -3, 4):
        for half in (0, 1):
            g_wait(o, d, half)

    acc[...] = jnp.zeros_like(acc)

    def group(d):
        def body(i, c):
            k = (i // 2) * 8 + yy[d] * 2 + lax.rem(i, 2)
            tail = qbuf[k, 2 * B : 2 * B + 72, :]
            tail = jnp.concatenate([tail[:, 32 * j : 32 * j + 32] for j in range(4)], axis=0)
            block = jnp.concatenate([qbuf[k, 0:B, :], qbuf[k, B : 2 * B, :], tail], axis=1)
            hi, lo = split(block)
            qh[k] = hi
            ql[k] = lo
            gh, gl = split(gbuf[k])
            acc[...] += dot3(hi, lo, gh, gl, ((0,), (0,)))
            return c

        lax.fori_loop(0, 4, body, 0)

    group(0)
    group(1)
    group(-1)

    on("N", lambda: n_b(2))
    for h in (0, 1):
        for c in (0, 1):
            q_wait(lambda: blk(h, 2, c), 0)
    on("S", lambda: s_far(2))
    group(2)

    on("S", lambda: rot_o.__setitem__(..., acc[...]))

    @pl.when(cond["N"])
    def _():
        send("N", lambda: acc, lambda: rot_o, lambda: us.at[2], "swap")

    arrived(mbuf.at[0], ms.at[0])
    arrived(mbuf.at[1], ms.at[1])
    rot = acc[...]
    new_first = 0.9 * mbuf[0] + 0.1 * rot
    new_second = 0.999 * mbuf[1] + 0.001 * rot * rot
    direction = new_first / bias_first / (jnp.sqrt(new_second / bias_second) + epsilon)
    hi, lo = split(direction)
    dh[...] = hi
    dl[...] = lo
    sums = jnp.broadcast_to(jnp.sum(direction * direction, axis=0, keepdims=True), (8, M))

    def product(c, d, buf):
        j = c * 8 + zz[d]
        buf[d % 8, 0:8, :] = sums
        buf[d % 8, 8:, :] = dot3(qh[j], ql[j], dh[...], dl[...], ((1,), (0,)))

    def other(d):
        product(o, d, osend)
        send(None, lambda: osend.at[d % 8], lambda: dbuf.at[d % 8], lambda: ds.at[d % 8], "core")

    def self_(d):
        product(b, d, ubuf)

    def chain(d):
        i = d % 8
        arrived(dbuf.at[i], ds.at[i])
        ways = {4: (("+", 0), ("-", 1)), 3: (("+", 0), ("+", 1)), 2: (("+", 0), ("+", 1)), 1: (("+", 0), ("+", 1))}
        todo = ways[d] if d > 0 else (("-", 1), ("-", 0))
        far_ = abs(d)

        def link(way, half):
            at, n = U_HALF[half]
            s = 0 if way == "+" else 1
            start = 4 if half == s else 3
            v = ubuf[i, at : at + n, :] + dbuf[i, at : at + n, :]
            if far_ < start:
                k = start - 1 - far_
                arrived(rbuf.at[s, half, k, pl.ds(0, n), :], rs.at[s, half, k])
                v = v + rbuf[s, half, k, 0:n, :]
            ubuf[i, at : at + n, :] = v
            k = start - far_
            send(
                None,
                lambda: ubuf.at[i, pl.ds(at, n), :],
                lambda: rbuf.at[s, half, k, pl.ds(0, n), :],
                lambda: rs.at[s, half, k],
                "z" + way,
            )

        for way, half in todo:
            link(way, half)

    other(4)
    self_(4)
    other(3)
    other(-3)
    chain(4)
    self_(3)
    self_(-3)
    chain(3)
    chain(-3)
    other(2)
    other(-2)
    self_(2)
    self_(-2)
    chain(2)
    chain(-2)
    other(1)
    other(-1)
    self_(1)
    self_(-1)
    other(0)
    self_(0)
    chain(1)
    chain(-1)

    arrived(dbuf.at[0], ds.at[0])

    def total(half):
        at, n = U_HALF[half]
        v = ubuf[0, at : at + n, :] + dbuf[0, at : at + n, :]
        for s in (0, 1):
            k = (4 if half == s else 3) - 1
            arrived(rbuf.at[s, half, k, pl.ds(0, n), :], rs.at[s, half, k])
            v = v + rbuf[s, half, k, 0:n, :]
        return v

    first = total(0)
    limit = jnp.maximum(1.0, jnp.sqrt(first[0:1] / D))

    def finish(half, v):
        def keep():
            upd_o[pl.ds(*G_HALF[half]), :] = v

        def hand():
            ustage[pl.ds(*G_HALF[half]), :] = v
            send(
                "N",
                lambda: ustage.at[pl.ds(*G_HALF[half]), :],
                lambda: upd_o.at[pl.ds(*G_HALF[half]), :],
                lambda: us.at[half],
                "swap",
            )

        on("S", keep)
        on("N", hand)

    finish(0, step_rate * first[8:] / limit)
    finish(1, step_rate * total(1) / limit)

    @pl.when(cond["N"])
    def _():
        arrived(rot_o, us.at[2])
        for half in (0, 1):
            arrived(upd_o.at[pl.ds(*G_HALF[half]), :], us.at[half])

    for tag in ("S", "N"):

        @pl.when(cond[tag])
        def _():
            for t, make in sends:
                if t == tag:
                    make().wait_send()

    for t, make in sends:
        if t is None:
            make().wait_send()


def solution(mesh):
    def step(gradient, first_moment, second_moment, weights, eigenbasis):
        m1, m2, w = first_moment.T, second_moment.T, weights.T
        f32, bf16 = jnp.float32, jnp.bfloat16
        vmem = pl.BlockSpec(memory_space=pltpu.VMEM)
        hbm = pl.BlockSpec(memory_space=pl.ANY)
        dma = pltpu.SemaphoreType.DMA
        rot, upd = pl.pallas_call(
            kernel,
            out_shape=[jax.ShapeDtypeStruct((B, M), f32)] * 2,
            in_specs=[vmem, vmem, hbm, hbm],
            out_specs=[vmem, vmem],
            scratch_shapes=[
                pltpu.VMEM((NB, B, M), f32),
                pltpu.VMEM((NB, 648, 128), f32),
                pltpu.VMEM((648, 128), f32),
                pltpu.VMEM((NB, B, B), bf16),
                pltpu.VMEM((NB, B, B), bf16),
                pltpu.VMEM((2, B, M), f32),
                pltpu.VMEM((B, M), f32),
                pltpu.VMEM((B, M), f32),
                pltpu.VMEM((B, M), bf16),
                pltpu.VMEM((B, M), bf16),
                pltpu.VMEM((8, B + 8, M), f32),
                pltpu.VMEM((8, B + 8, M), f32),
                pltpu.VMEM((8, B + 8, M), f32),
                pltpu.VMEM((2, 2, 4, 152, M), f32),
                dma((NSEND,)),
                dma((NB, 2)),
                dma((NB, 2)),
                dma((2,)),
                dma((8,)),
                dma((2, 2, 4)),
                dma((3,)),
            ],
            compiler_params=pltpu.CompilerParams(collective_id=0, has_side_effects=True, vmem_limit_bytes=56 * 2**20),
        )(gradient.T, eigenbasis, m1, m2)
        new_first = 0.9 * m1 + 0.1 * rot
        new_second = 0.999 * m2 + 0.001 * rot * rot
        new_weights = w - upd
        return new_weights.T, new_first.T, new_second.T

    spec = P("row", "col")
    return jax.shard_map(step, mesh=mesh, in_specs=(spec,) * 5, out_specs=(spec,) * 3, check_vma=False)
```

```python
import jax
import jax.numpy as jnp
from jax import lax
from jax.experimental import pallas as pl
from jax.experimental.pallas import tpu as pltpu
from jax.sharding import PartitionSpec as P

MESH = pl.DeviceIdType.MESH
D = 4608
bias_first = 1.0 - 0.9**10
bias_second = 1.0 - 0.999**10
epsilon = 1e-08
step_rate = 0.25

B = 288
M = 256
NB = 16
Q_HALF = ((0, 376), (376, 272))
G_PART = ((0, 72), (72, 72), (144, 72), (216, 72))
U_PART = ((0, 80), (80, 72), (152, 72), (224, 72))
FAR_SIDE = ((0, 1), (2, 3))
NSEND = 288


def split(v):
    hi = v.astype(jnp.bfloat16)
    return hi, (v - hi.astype(jnp.float32)).astype(jnp.bfloat16)


def dot(p, q):
    return jnp.dot(p, q, preferred_element_type=jnp.float32)


def kernel(g, q, m1, m2, rot_o, upd_o, gbuf, qbuf, qstage, qcat, tcat, mbuf, acc, pbuf, dcat, osend, ubuf, dbuf, rbuf, ss, qs, gs, ms, ds, rs, ps, us):
    row, col = lax.axis_index("row"), lax.axis_index("col")
    xh, y, b = row // 8, lax.rem(row // 2, 4), lax.rem(row, 2)
    a, z = col // 8, lax.rem(col, 8)
    x = 2 * xh + a
    o = 1 - b
    cond = {"S": a == b, "N": a != b}
    yy = {d: lax.rem(y + d + 4, 4) for d in (0, 1, -1, 2)}
    zz = {d: lax.rem(z + d + 8, 8) for d in range(-4, 5)}

    def dev(x_, y_, z_, c_):
        return ((x_ // 2) * 8 + y_ * 2 + c_, lax.rem(x_, 2) * 8 + z_)

    px, qx = 2 * xh + 1 - a, lax.rem(x + 2 * a + 3, 4)
    to = {
        "p": dev(px, y, z, b),
        "q": dev(qx, y, z, b),
        "y+": dev(x, yy[1], z, b),
        "y-": dev(x, yy[-1], z, b),
        "z+": dev(x, y, zz[1], b),
        "z-": dev(x, y, zz[-1], b),
        "core": dev(x, y, z, o),
        "swap": dev(2 * xh + b, y, z, o),
        "s+": dev(2 * xh + b, y, zz[1], o),
        "s-": dev(2 * xh + b, y, zz[-1], o),
    }

    def on(tag, f):
        if tag is None:
            f()
        else:
            pl.when(cond[tag])(f)

    sends = []

    def send(tag, src, dst, rsem, where):
        k = len(sends)

        def make():
            return pltpu.make_async_remote_copy(
                src_ref=src(), dst_ref=dst(), send_sem=ss.at[k], recv_sem=rsem(), device_id=to[where], device_id_type=MESH
            )

        make().start()
        sends.append((tag, make))

    def arrived(ref, sem):
        pltpu.make_async_copy(ref, ref, sem).wait()

    def blk(h, d, k):
        return h * 8 + yy[d] * 2 + (o if k else b)

    def near(d, k):
        return lambda: blk(xh, d, k)

    def far(d, k):
        return lambda: blk(1 - xh, d, k)

    def q_part(i, half):
        return qbuf.at[i, pl.ds(*Q_HALF[half]), :]

    def q_send(tag, i, half, *wheres):
        for w in wheres:
            send(tag, lambda: q_part(i(), half), lambda: q_part(i(), half), lambda: qs.at[i(), half], w)

    def q_wait(i, half):
        arrived(q_part(i(), half), qs.at[i(), half])

    def g_part(c, d, half):
        return gbuf.at[c * 8 + zz[d], pl.ds(*G_PART[half]), :]

    def g_send(tag, d, half, *wheres, src=None):
        for w in wheres:
            s = (lambda: g.at[pl.ds(*G_PART[half]), :]) if src else (lambda: g_part(b, d, half))
            send(tag, s, lambda: g_part(b, d, half), lambda: gs.at[b * 8 + zz[d], half], w)

    def g_wait(c, d, half):
        arrived(g_part(c, d, half), gs.at[c * 8 + zz[d], half])

    def pack(put):
        put(0, B, q[:, 0:128])
        put(B, B, q[:, 128:256])
        put(2 * B, 72, jnp.concatenate([q[72 * i : 72 * i + 72, 256:288] for i in range(4)], axis=1))

    def pack_own():
        def put(at, n, v):
            qbuf[row, at : at + n, :] = v

        pack(put)

    def pack_stage():
        def put(at, n, v):
            qstage[at : at + n, :] = v

        pack(put)

    barrier = pltpu.get_barrier_semaphore()

    def greet(*wheres):
        for w in wheres:
            pl.semaphore_signal(barrier, inc=1, device_id=to[w], device_id_type=MESH)

    greet("p", "q", "y+", "y-", "z+", "z-", "core")
    on("N", lambda: greet("swap", "s+", "s-"))
    on("S", pack_own)
    on("N", pack_stage)
    on("S", lambda: pl.semaphore_wait(barrier, 7))
    on("N", lambda: pl.semaphore_wait(barrier, 10))

    own, mate = near(0, 0), near(0, 1)

    def local(half):
        return pltpu.make_async_copy(g.at[pl.ds(*G_PART[half]), :], g_part(b, 0, half), gs.at[b * 8 + z, half])

    def s_first():
        q_send("S", own, 0, "p", "q")
        q_send("S", own, 1, "y+", "y-")
        for j in (0, 1):
            for t in (0, 1):
                g_send("S", 0, FAR_SIDE[t][j], *(("z+", "z-") if t == 0 else ("z-", "z+")), "core", src=True)
        for part in range(4):
            local(part).start()
        pltpu.make_async_copy(m1, mbuf.at[0], ms.at[0]).start()
        pltpu.make_async_copy(m2, mbuf.at[1], ms.at[1]).start()
        q_wait(mate, 0)
        q_send("S", mate, 0, "p", "q")
        q_wait(mate, 1)
        q_send("S", mate, 1, "y-", "y+")
        q_send("S", own, 1, "p", "q")
        q_send("S", own, 0, "y+", "y-")
        q_send("S", mate, 1, "p", "q")
        q_send("S", mate, 0, "y-", "y+")

    def n_first():
        def hand_q(half):
            send("N", lambda: qstage.at[pl.ds(*Q_HALF[half]), :], lambda: q_part(row, half), lambda: qs.at[row, half], "core")

        def hand_g(half):
            send("N", lambda: g.at[pl.ds(*G_PART[half]), :], lambda: g_part(o, 0, half), lambda: gs.at[o * 8 + z, half], "swap")

        hand_q(0)
        hand_q(1)
        for part in (0, 2, 1, 3):
            hand_g(part)

        def first(i, *wheres):
            q_wait(i, 0)
            q_send("N", i, 0, *wheres)

        def ring(half):
            g_wait(b, 0, half)
            g_send("N", 0, half, "z+", "z-", "core")

        ring(0)
        ring(2)
        first(near(0, 0), "q", "y+", "y-")
        first(far(0, 0), "y+", "y-")
        ring(1)
        ring(3)
        first(far(0, 1), "p", "y-", "y+")
        first(near(0, 1), "y-", "y+")

    def s_columns():
        for i, way in ((near(-1, 0), "y+"), (near(1, 1), "y-"), (near(-1, 1), None), (near(1, 0), None)):
            q_wait(i, 1)
            if way:
                q_send("S", i, 1, way)
            q_send("S", i, 1, "p", "q")

    def s_rows():
        q_wait(far(0, 0), 0)
        q_send("S", far(0, 0), 0, "y+", "y-")
        q_wait(far(0, 1), 0)
        q_send("S", far(0, 1), 0, "y-", "y+")

    def z_event(tag, d):
        for fresh in (False, True):
            for j in (0, 1):
                for t, way in enumerate("+-"):
                    part = FAR_SIDE[1 - t if fresh else t][j]
                    hops = 3 if fresh else 4
                    back = d if t else -d
                    if d <= hops:
                        g_wait(b, back, part)
                        g_send(tag, back, part, *((["z" + way] if d < hops else []) + ["core"]))

    def n_columns(d):
        for k in (0, 1):
            q_wait(near(d, k), 1)
            if (d, k) != (0, 1):
                q_send("N", near(d, k), 1, "q")
            q_wait(far(d, k), 1)
            if (d, k) == (0, 1):
                q_send("N", far(d, k), 1, "p")

    def a_ring(tag, h, k):
        for d, way in ((-1, "y+"), (1, "y-")):
            q_wait(h(d, k), 0)
            if way == ("y+", "y-")[k]:
                q_send(tag, h(d, k), 0, way)

    def s_columns_far():
        for k in (0, 1):
            q_wait(near(2, k), 1)
            q_send("S", near(2, k), 1, "p", "q")

    def s_wait(d):
        for k in (0, 1):
            q_wait(far(d, k), 1)

    def moments():
        send("N", lambda: m1, lambda: mbuf.at[0], lambda: ms.at[0], "swap")
        send("N", lambda: m2, lambda: mbuf.at[1], lambda: ms.at[1], "swap")

    def prep(h, *shifts):
        def body(i, carry):
            d = jnp.where(i // 2 == 0, yy[shifts[0]], yy[shifts[-1]])
            k = h * 8 + d * 2 + lax.rem(i, 2)
            tail = qbuf[k, 2 * B : 2 * B + 72, :]
            tail = jnp.concatenate([tail[:, 32 * j : 32 * j + 32] for j in range(4)], axis=0)
            main = jnp.concatenate([qbuf[k, 0:B, :], qbuf[k, B : 2 * B, :]], axis=1)
            hi, lo = split(main)
            tail_hi = tail.astype(jnp.bfloat16).astype(jnp.float32)
            ends = jnp.concatenate([tail_hi, tail_hi, tail - tail_hi], axis=1).astype(jnp.bfloat16)
            qcat[k, :, 0:256] = hi
            qcat[k, :, 256:512] = hi
            qcat[k, :, 512:768] = lo
            qcat[k, :, 768:864] = ends
            hi, lo = split(jnp.concatenate([main, tail], axis=1))
            tcat[k] = jnp.concatenate([hi, hi, lo], axis=0).T
            return carry

        lax.fori_loop(0, 2 * len(shifts), body, 0, unroll=2)

    def group(h, *shifts):
        def body(i, carry):
            d = jnp.where(i // 2 == 0, yy[shifts[0]], yy[shifts[-1]])
            k = h * 8 + d * 2 + lax.rem(i, 2)
            gh, gl = split(gbuf[k])
            acc[...] += dot(tcat[k], jnp.concatenate([gh, gl, gh], axis=0))
            return carry

        lax.fori_loop(0, 2 * len(shifts), body, 0, unroll=2)

    acc[...] = jnp.zeros_like(acc)
    def s_order():
        s_first()
        s_columns()
        z_event("S", 1)
        a_ring("S", near, 0)
        a_ring("S", near, 1)
        s_columns_far()
        z_event("S", 2)
        s_rows()
        prep(xh, 0)
        z_event("S", 3)
        prep(xh, 1, -1)
        a_ring("S", far, 0)
        z_event("S", 4)
        a_ring("S", far, 1)
        for d in (0, 1, -1):
            s_wait(d)
        prep(1 - xh, 0)
        prep(1 - xh, 1, -1)

    def n_order():
        n_first()
        z_event("N", 1)
        n_columns(0)
        a_ring("N", near, 0)
        prep(xh, 0)
        z_event("N", 2)
        n_columns(-1)
        n_columns(1)
        a_ring("N", far, 0)
        a_ring("N", far, 1)
        moments()
        z_event("N", 3)
        a_ring("N", near, 1)
        n_columns(2)
        prep(xh, 1, -1)
        prep(1 - xh, 0)
        prep(1 - xh, 1, -1)
        z_event("N", 4)

    on("S", s_order)
    on("N", n_order)
    for part in range(4):
        on("S", lambda: g_wait(b, 0, part))
    for d in (0, 1, -1, 2, -2, 3, -3, 4):
        for part in range(4):
            g_wait(o, d, part)
    group(xh, 0)
    group(xh, 1, -1)
    group(1 - xh, 0)
    group(1 - xh, 1, -1)
    for k in (0, 1):
        q_wait(near(2, k), 0)
    prep(xh, 2)
    group(xh, 2)
    for k in (0, 1):
        q_wait(far(2, k), 0)
    on("S", lambda: s_wait(2))
    prep(1 - xh, 2)
    group(1 - xh, 2)

    on("S", lambda: rot_o.__setitem__(..., acc[...]))

    @pl.when(cond["N"])
    def _():
        send("N", lambda: acc, lambda: rot_o, lambda: us.at[0], "swap")

    arrived(mbuf.at[0], ms.at[0])
    arrived(mbuf.at[1], ms.at[1])
    rot = acc[...]
    new_first = 0.9 * mbuf[0] + 0.1 * rot
    new_second = 0.999 * mbuf[1] + 0.001 * rot * rot
    direction = new_first / bias_first / (jnp.sqrt(new_second / bias_second) + epsilon)
    hi, lo = split(direction)
    for at, part in enumerate((hi, lo, hi)):
        dcat[256 * at : 256 * at + 256, :] = part[0:256]
        dcat[768 + 32 * at : 800 + 32 * at, :] = part[256:288]
    sums = jnp.broadcast_to(jnp.sum(direction * direction, axis=0, keepdims=True), (8, M))

    def product(c, d, buf):
        j = c * 8 + zz[d]
        buf[d % 8, 0:8, :] = sums
        buf[d % 8, 8:, :] = dot(qcat[j], dcat[...])

    def other(d):
        product(o, d, osend)
        send(None, lambda: osend.at[d % 8], lambda: dbuf.at[d % 8], lambda: ds.at[d % 8], "core")

    def self_(d):
        product(b, d, ubuf)

    def core_sum(*ds_):
        for d in ds_:
            arrived(dbuf.at[d % 8], ds.at[d % 8])

    def came(s, c, k):
        n = U_PART[c][1]
        arrived(rbuf.at[s, c, k, pl.ds(0, n), :], rs.at[s, c, k])
        return rbuf[s, c, k, 0:n, :]

    def link(d, s, c):
        i, (at, n) = d % 8, U_PART[c]
        start = 4 if c in FAR_SIDE[s] else 3
        k = start - abs(d)
        v = ubuf[i, at : at + n, :] + dbuf[i, at : at + n, :]
        if k:
            v = v + came(s, c, k - 1)
        ubuf[i, at : at + n, :] = v

        def go(tag, where):
            send(
                tag,
                lambda: ubuf.at[i, pl.ds(at, n), :],
                lambda: rbuf.at[s, c, k, pl.ds(0, n), :],
                lambda: rs.at[s, c, k],
                where + "+-"[s],
            )

        if abs(d) > 1:
            go(None, "z")
        else:
            on("S", lambda: go("S", "z"))
            on("N", lambda: go("N", "s"))

    def links(d, fresh):
        for j in (0, 1):
            for s in (0, 1):
                link(d if s == 0 else -d, s, FAR_SIDE[1 - s if fresh else s][j])

    other(4)
    self_(4)
    other(3)
    other(-3)
    core_sum(4)
    for j in (0, 1):
        for s in (0, 1):
            link(4, s, FAR_SIDE[s][j])
    self_(3)
    self_(-3)
    core_sum(3, -3)
    links(3, True)
    other(0)
    self_(0)
    other(2)
    other(-2)
    self_(2)
    self_(-2)
    core_sum(0)

    @pl.when(cond["S"])
    def _():
        pbuf[...] = ubuf[0] + dbuf[0]

    @pl.when(cond["N"])
    def _():
        ubuf[0] = ubuf[0] + dbuf[0]
        send("N", lambda: ubuf.at[0], lambda: pbuf, lambda: ps.at[0], "swap")

    links(3, False)
    core_sum(2, -2)
    links(2, True)
    other(1)
    other(-1)
    self_(1)
    self_(-1)
    links(2, False)
    core_sum(1, -1)
    links(1, True)
    links(1, False)
    on("N", lambda: arrived(pbuf, ps.at[0]))

    limit = None
    for c, (at, n) in enumerate(U_PART):
        v = pbuf[at : at + n, :]
        for s in (0, 1):
            v = v + came(s, c, 3 if c in FAR_SIDE[s] else 2)
        if c == 0:
            limit = jnp.maximum(1.0, jnp.sqrt(v[0:1] / D))
            v = v[8:]
        upd_o[72 * c : 72 * c + 72, :] = step_rate * v / limit

    on("N", lambda: arrived(rot_o, us.at[0]))

    for tag in ("S", "N"):

        @pl.when(cond[tag])
        def _():
            for t, make in sends:
                if t == tag:
                    make().wait_send()

    for t, make in sends:
        if t is None:
            make().wait_send()


def solution(mesh):
    def step(gradient, first_moment, second_moment, weights, eigenbasis):
        m1, m2, w = first_moment.T, second_moment.T, weights.T
        f32, bf16 = jnp.float32, jnp.bfloat16
        vmem = pl.BlockSpec(memory_space=pltpu.VMEM)
        hbm = pl.BlockSpec(memory_space=pl.ANY)
        dma = pltpu.SemaphoreType.DMA
        rot, upd = pl.pallas_call(
            kernel,
            out_shape=[jax.ShapeDtypeStruct((B, M), f32)] * 2,
            in_specs=[vmem, vmem, hbm, hbm],
            out_specs=[vmem, vmem],
            scratch_shapes=[
                pltpu.VMEM((NB, B, M), f32),
                pltpu.VMEM((NB, 648, 128), f32),
                pltpu.VMEM((648, 128), f32),
                *[pltpu.VMEM((NB, B, 3 * B), bf16)] * 2,
                pltpu.VMEM((2, B, M), f32),
                pltpu.VMEM((B, M), f32),
                pltpu.VMEM((B + 8, M), f32),
                pltpu.VMEM((3 * B, M), bf16),
                pltpu.VMEM((8, B + 8, M), f32),
                pltpu.VMEM((8, B + 8, M), f32),
                pltpu.VMEM((8, B + 8, M), f32),
                pltpu.VMEM((2, 4, 4, 80, M), f32),
                dma((NSEND,)),
                dma((NB, 2)),
                dma((NB, 4)),
                dma((2,)),
                dma((8,)),
                dma((2, 4, 4)),
                dma((1,)),
                dma((1,)),
            ],
            compiler_params=pltpu.CompilerParams(collective_id=0, has_side_effects=True, vmem_limit_bytes=56 * 2**20),
        )(gradient.T, eigenbasis, m1, m2)
        new_first = 0.9 * m1 + 0.1 * rot
        new_second = 0.999 * m2 + 0.001 * rot * rot
        new_weights = w - upd
        return new_weights.T, new_first.T, new_second.T

    spec = P("row", "col")
    return jax.shard_map(step, mesh=mesh, in_specs=(spec,) * 5, out_specs=(spec,) * 3, check_vma=False)
```
